256 devices in a mesh: head: 2 (over core), outer: 16 (over x, y), inner: 8 (over z).
Axes of the slice: x: 4, y: 4, z: 8, core: 2. Of those that a mesh axis runs over, the one named last changes fastest.
Arguments:
- queries: bfloat16 [65536, 2048], P(('outer', 'inner'), 'head'), may hold values from -6 to 6
- key_rows: bfloat16 [65536, 2048], P(('outer', 'inner'), 'head'), may hold values from -6 to 6
- value_rows: bfloat16 [65536, 2048], P(('outer', 'inner'), 'head'), may hold values from -6 to 6
- teacher_out: bfloat16 [65536, 2048], P(('outer', 'inner'), 'head'), may hold values from -6 to 6
- level_weights: bfloat16 [8, 65536], P(None, ('outer', 'inner')), may hold values from 0.125 to 1
Outputs:
- grad_queries: bfloat16 [65536, 2048], P(('outer', 'inner'), 'head')
- grad_keys: bfloat16 [65536, 2048], P(('outer', 'inner'), 'head')
- grad_values: bfloat16 [65536, 2048], P(('outer', 'inner'), 'head')
- grad_levels: float32 [8, 65536], P(None, ('outer', 'inner'))
The draws below stay inside these ranges and needn't reach their ends.
All inputs are finite; a program needn't handle non-finite values.
Results may differ from the reference program's by a relative error of at most 0.014.
Values may be sent and summed in bfloat16 or wider, within the bound.
A program may use at most 128 MiB of HBM per device.

```python
import math
import jax
import jax.numpy as jnp
from jax import lax

TOK_DEV = 512
HEADS = 16
DK = 128
LEVELS = 8
SPANS = 128
TOKENS = 65536
BITS_IN = 3
BITS_OUT = 4
N_OUTER = 16
N_INNER = 8


def steps_of(rng, shape, cuts, least, high):
    def one(dim, parts):
        steps = jax.random.uniform(jax.random.fold_in(jax.random.fold_in(rng, 6), dim), (parts,), jnp.float32, least / len(cuts), high / len(cuts))
        return jnp.repeat(jnp.exp(steps), shape[dim] // parts).reshape((-1,) + (1,) * (len(shape) - dim - 1))

    factor_of = one(*cuts[0])
    for cut in cuts[1:]:
        factor_of = factor_of * one(*cut)
    return factor_of


def bell_draw(key, dims, spread, reach, split=(), kind=jnp.bfloat16):
    result = jax.random.normal(key, dims, jnp.float32) * spread
    if len(split) > 0:
        result = steps_of(key, dims, split, -0.22, 0.18) * result
    return jnp.clip(result, min=-reach, max=reach).astype(kind)


def setup_inputs(seed: int = 0) -> dict:
    key_of = jax.random.split(jax.random.key(seed), 6)
    queries = bell_draw(key_of[0], (TOKENS, HEADS * DK), 1.0, 6.0, ((0, 128), (1, 2)))
    key_rows = bell_draw(key_of[1], (TOKENS, HEADS * DK), 1.0, 6.0, ((0, 128), (1, 2)))
    value_rows = bell_draw(key_of[2], (TOKENS, HEADS * DK), 1.0, 6.0, ((0, 128), (1, 2)))
    teacher_out = bell_draw(key_of[3], (TOKENS, HEADS * DK), 1.0, 6.0, ((0, 128), (1, 2)))
    level_weights = jnp.clip(jnp.exp(math.log(1.0) - 2.0794415 * jax.random.uniform(key_of[4], (LEVELS, TOKENS), jnp.float32) ** steps_of(key_of[4], (LEVELS, TOKENS), ((1, 128),), -0.2, 0.2)), 0.125, 1.0).astype(jnp.bfloat16)
    return {"queries": queries, "key_rows": key_rows, "value_rows": value_rows, "teacher_out": teacher_out, "level_weights": level_weights}


HIGH = lax.Precision.HIGHEST


def bit_of(number, position):
    return (number >> position) % 2


def level_masks(block_id, forward):
    inner_pos = block_id % N_INNER
    group_pos = block_id // N_INNER
    members = jnp.arange(N_INNER, dtype=jnp.int32)
    groups_all = jnp.arange(N_OUTER, dtype=jnp.int32)
    own_bit = 1 if forward else 0
    rows_in = []
    rows_out = []
    for level_num in range(1, LEVELS):
        bit_pos = level_num - 1
        if bit_pos < BITS_IN:
            chosen = (bit_of(inner_pos, bit_pos) == own_bit) & ((members >> level_num) == (inner_pos >> level_num)) & (bit_of(members, bit_pos) == 1 - own_bit)
            rows_in.append(chosen)
            rows_out.append(jnp.zeros((N_OUTER,), dtype=bool))
        else:
            outer_bit = bit_pos - BITS_IN
            chosen = (bit_of(group_pos, outer_bit) == own_bit) & ((groups_all >> (outer_bit + 1)) == (group_pos >> (outer_bit + 1))) & (bit_of(groups_all, outer_bit) == 1 - own_bit)
            if outer_bit >= BITS_OUT:
                chosen = jnp.zeros((N_OUTER,), dtype=bool)
            rows_in.append(jnp.zeros((N_INNER,), dtype=bool))
            rows_out.append(chosen)
    return jnp.stack(rows_in).astype(jnp.float32), jnp.stack(rows_out).astype(jnp.float32)


def to_low(array):
    return lax.optimization_barrier(array.astype(jnp.bfloat16)).astype(jnp.float32)


def reference(queries, key_rows, value_rows, teacher_out, level_weights):
    gamma = DK ** -0.5
    scale_list = [TOK_DEV ** -0.5] + [gamma * (TOK_DEV * 2 ** (num - 1)) ** -0.5 for num in range(1, LEVELS)]
    scales = jnp.array(scale_list, dtype=jnp.float32)
    query_blocks = queries.reshape(SPANS, TOK_DEV, HEADS, DK)
    key_blocks = key_rows.reshape(SPANS, TOK_DEV, HEADS, DK)
    value_blocks = value_rows.reshape(SPANS, TOK_DEV, HEADS, DK)
    teacher_blocks = teacher_out.reshape(SPANS, TOK_DEV, HEADS, DK)
    weight_blocks = level_weights.reshape(LEVELS, SPANS, TOK_DEV).transpose(1, 0, 2)
    block_ids = jnp.arange(SPANS, dtype=jnp.int32)

    def state_of(index):
        keys32 = key_blocks[index].astype(jnp.float32)
        values32 = value_blocks[index].astype(jnp.float32)
        return jnp.einsum('thd,the->hde', keys32, values32).astype(jnp.bfloat16)

    block_states = lax.map(state_of, block_ids)
    group_totals = block_states.astype(jnp.float32).reshape(N_OUTER, N_INNER, HEADS, DK, DK).sum(axis=1).astype(jnp.bfloat16)
    totals32 = group_totals.astype(jnp.float32)
    positions = jnp.arange(TOK_DEV, dtype=jnp.int32)
    lower = positions[:, None] >= positions[None, :]

    def first_pass(index):
        in_mask, out_mask = level_masks(index, True)
        group_pos = index // N_INNER
        group_states = lax.dynamic_slice_in_dim(block_states, (group_pos * N_INNER).astype(jnp.int32), N_INNER, 0).astype(jnp.float32)
        level_state = jnp.einsum('lj,jhde->lhde', in_mask, group_states, precision=HIGH) + jnp.einsum('lg,ghde->lhde', out_mask, totals32, precision=HIGH)
        state32 = to_low(level_state)
        query32 = query_blocks[index].astype(jnp.float32)
        key32 = key_blocks[index].astype(jnp.float32)
        value32 = value_blocks[index].astype(jnp.float32)
        teacher32 = teacher_blocks[index].astype(jnp.float32)
        coefs = weight_blocks[index].astype(jnp.float32) * scales[:, None]
        scores = gamma * jnp.einsum('thd,shd->hts', query32, key32)
        scores32 = to_low(jnp.where(lower[None], scores, 0.0))
        intra = jnp.einsum('hts,she->the', scores32, value32)
        reads = jnp.einsum('thd,lhde->lthe', query32, state32)
        student = coefs[0][:, None, None] * intra + jnp.sum(coefs[1:, :, None, None] * reads, axis=0)
        error32 = to_low(student - teacher32)
        back_reads = jnp.einsum('the,lhde->lthd', error32, state32)
        grad_first = scales[0] * jnp.sum(error32 * intra, axis=(1, 2))
        grad_rest = scales[1:, None] * jnp.sum(query32[None] * back_reads, axis=(2, 3))
        grad_lv = jnp.concatenate([grad_first[None], grad_rest], axis=0)
        intra_err = to_low(coefs[0][:, None, None] * error32)
        score_grad = to_low(jnp.where(lower[None], gamma * jnp.einsum('the,she->hts', intra_err, value32), 0.0))
        grad_q = jnp.einsum('hts,shd->thd', score_grad, key32) + jnp.sum(coefs[1:, :, None, None] * back_reads, axis=0)
        exists = bit_of(index, jnp.arange(LEVELS - 1, dtype=jnp.int32)).astype(jnp.float32)
        weighted = to_low((coefs[1:] * exists[:, None])[:, :, None, None] * error32[None])
        adjoint = jnp.einsum('thd,lthe->lhde', query32, weighted)
        key_part = jnp.einsum('hts,thd->shd', score_grad, query32)
        value_part = jnp.einsum('hts,the->she', scores32, intra_err)
        return grad_q.astype(jnp.bfloat16), grad_lv, adjoint, key_part, value_part

    grad_q_all, grad_lv_all, adjoints, key_parts, value_parts = lax.map(first_pass, block_ids)
    group_adjoint = adjoints.reshape(N_OUTER, N_INNER, LEVELS - 1, HEADS, DK, DK).sum(axis=1)

    def second_pass(index):
        in_mask, out_mask = level_masks(index, False)
        group_pos = index // N_INNER
        group_adj = lax.dynamic_slice_in_dim(adjoints, (group_pos * N_INNER).astype(jnp.int32), N_INNER, 0)
        total = jnp.einsum('lj,jlhde->hde', in_mask, group_adj, precision=HIGH) + jnp.einsum('lg,glhde->hde', out_mask, group_adjoint, precision=HIGH)
        adjoint32 = to_low(total)
        key32 = key_blocks[index].astype(jnp.float32)
        value32 = value_blocks[index].astype(jnp.float32)
        grad_k = key_parts[index] + jnp.einsum('hde,she->shd', adjoint32, value32)
        grad_v = value_parts[index] + jnp.einsum('hde,shd->she', adjoint32, key32)
        return grad_k.astype(jnp.bfloat16), grad_v.astype(jnp.bfloat16)

    grad_k_all, grad_v_all = lax.map(second_pass, block_ids)
    grad_queries = grad_q_all.reshape(TOKENS, HEADS * DK)
    grad_keys = grad_k_all.reshape(TOKENS, HEADS * DK)
    grad_values = grad_v_all.reshape(TOKENS, HEADS * DK)
    grad_levels = grad_lv_all.transpose(1, 0, 2).reshape(LEVELS, TOKENS)
    return grad_queries, grad_keys, grad_values, grad_levels
```

```python
import functools

import jax
import jax.numpy as jnp
from jax import lax
from jax.experimental import pallas as pl
from jax.experimental.pallas import tpu as pltpu
from jax.sharding import PartitionSpec as P

DK = 128
MESH = pl.DeviceIdType.MESH
F32 = jnp.float32
BF16 = jnp.bfloat16


def nn(a, b):
    return lax.dot_general(a, b, (((1,), (0,)), ((), ())), preferred_element_type=F32)


def nt(a, b):
    return lax.dot_general(a, b, (((1,), (1,)), ((), ())), preferred_element_type=F32)


def tn(a, b):
    return lax.dot_general(a, b, (((0,), (0,)), ((), ())), preferred_element_type=F32)


def bit_of(number, position):
    return lax.rem(lax.div(number, 2**position), 2)


def kernel(
    dims,
    q_hbm, k_hbm, v_hbm, y_hbm, w_hbm,
    gq_hbm, gk_hbm, gv_hbm, gl_hbm,
    Q, K, V, Y, W, BS, FR, LS, IS, TOT, YR, YT, XR, COEF, QC, SC, IN, ER, AD,
    AL1, AI, RP, BXS, BXR, BYS, BYR, DS, BA, GK, GV, OQ, OK, OV, GACC, GLP, GLR,
    in_sem, w_sem, out_sem, gl_sem,
    f1s, f1r, fl1, f2s, f2r, fys, fyr, fxs, fxr, f3s, f3r,
    bl1, b2s, b2r, b3s, b3r, bxs, bxr, bys, byr, b4s, b4r, glx,
):
    n, nlo, nhi, nhead, ib, lob, hib, rows, scales, gamma = dims
    ob = lob + hib
    nb = ib + ob
    half = n // 2
    p = lax.axis_index("inner")
    g = lax.axis_index("outer")
    hd = lax.axis_index("head")
    x = lax.div(g, nlo)
    y = lax.rem(g, nlo)

    def zdev(r):
        return (hd, g, r)

    def odev(o):
        return (hd, o, p)

    def ydev(yy):
        return odev(x * nlo + yy)

    def xdev(xx):
        return odev(xx * nlo + y)

    def wrap(i):
        return lax.rem(i + 2 * n, n)

    def loop(count, body, unroll=1):
        def step(i, c):
            body(i)
            return c
        lax.fori_loop(0, count, step, 0, unroll=unroll)

    def rc(src, dst, ss, rs, dev):
        return pltpu.make_async_remote_copy(
            src_ref=src, dst_ref=dst, send_sem=ss, recv_sem=rs, device_id=dev, device_id_type=MESH
        )

    def cols(h):
        return pl.ds(pl.multiple_of(h * DK, DK), DK)

    def lev(b):
        return pl.ds(b * DK, DK)

    def in_copy(a, h):
        hbm, vm = ((k_hbm, K), (v_hbm, V), (q_hbm, Q), (y_hbm, Y))[a]
        return pltpu.make_async_copy(hbm.at[:, cols(h)], vm.at[h], in_sem.at[a, h])

    def out_copy(a, h):
        hbm, vm = ((gq_hbm, OQ), (gk_hbm, OK), (gv_hbm, OV))[a]
        return pltpu.make_async_copy(vm.at[h], hbm.at[:, cols(h)], out_sem.at[a, h])

    def start_kv(h):
        in_copy(0, h).start()
        in_copy(1, h).start()

    def start_qy(h):
        in_copy(2, h).start()
        in_copy(3, h).start()

    loop(n, start_kv)
    w_copy = pltpu.make_async_copy(w_hbm, W, w_sem)
    w_copy.start()
    loop(n, start_qy)

    barrier = pltpu.get_barrier_semaphore()

    def greet(dev):
        pl.semaphore_signal(barrier, inc=1, device_id=dev, device_id_type=MESH)

    loop(n - 1, lambda i: greet(zdev(wrap(p + 1 + i))))
    loop(nlo - 1, lambda i: greet(ydev(lax.rem(y + 1 + i, nlo))))
    loop(nhi - 1, lambda i: greet(xdev(lax.rem(x + 1 + i, nhi))))
    if nhead == 2:
        greet((1 - hd, g, p))

    def state(i):
        h = wrap(p + half + i)
        in_copy(0, h).wait()
        in_copy(1, h).wait()
        BS[h] = tn(K[h], V[h]).astype(BF16)

    loop(n, state, unroll=2)
    pl.semaphore_wait(barrier, (n - 1) + (nlo - 1) + (nhi - 1) + (nhead - 1))

    def f1(h, src):
        return rc(BS.at[h], FR.at[src], f1s.at[h], f1r.at[src], zdev(h))

    def f1_start(i):
        f1(wrap(p + half + i), p).start()

    loop(half, f1_start)
    loop(half - 1, lambda i: f1(wrap(p + 1 + i), p).start())
    fl1_copy = rc(BS, LS.at[:, lev(0), :], fl1.at[0], fl1.at[1], zdev(wrap(p + 1)))
    low0 = bit_of(p, 0) == 0

    @pl.when(low0)
    def _():
        fl1_copy.start()

    FR[p] = BS[p]

    w_copy.wait()
    for b in range(nb):
        bit = bit_of(p, b) if b < ib else bit_of(g, b - ib)

        @pl.when(bit == 0)
        def _():
            LS[:, lev(b), :] = jnp.zeros((n, DK, DK), BF16)

    weights = W[...]
    pick = lax.broadcasted_iota(jnp.int32, (nb + 1, DK), 0)
    for num in range(nb + 1):
        COEF[num] = tn(weights, jnp.where(pick == num, 1.0, 0.0).astype(BF16)) * scales[num]
    GACC[...] = jnp.zeros_like(GACC)

    def lower():
        return lax.broadcasted_iota(jnp.int32, (rows, rows), 0) >= lax.broadcasted_iota(
            jnp.int32, (rows, rows), 1
        )

    def ahead(h):
        in_copy(2, h).wait()
        in_copy(3, h).wait()
        query = Q[h]
        scores = nt(query, K[h]) * gamma
        kept = jnp.where(lower(), scores, 0.0).astype(BF16)
        SC[h] = kept
        IN[h] = nn(kept, V[h])
        query32 = query.astype(F32)
        for b in range(nb):
            QC[h, :, lev(b)] = (query32 * COEF[b + 1]).astype(BF16)

    loop(n, ahead)

    def f1_wait(i):
        src = wrap(p + 1 + i)
        f1(src, src).wait_recv()

    loop(n - 1, f1_wait)
    states = [FR[i].astype(F32) for i in range(n)]
    total = sum(states[1:], states[0])
    TOT[...] = total.astype(BF16)
    for b in range(1, ib):
        for node in range(n // 2 ** (b + 1)):
            first = node * 2 ** (b + 1)
            members = states[first : first + 2**b]
            IS[b - 1, node] = sum(members[1:], members[0]).astype(BF16)
    YR[y] = TOT[...]

    def fy(j, src):
        return rc(TOT, YR.at[src], fys.at[j], fyr.at[src], ydev(lax.rem(y + 1 + j, nlo)))

    loop(nlo - 1, lambda j: fy(j, y).start())

    def f2(b, dst, src):
        node = lax.div(dst, 2 ** (b + 1))
        return rc(
            IS.at[b - 1, node], LS.at[src, lev(b), :], f2s.at[b - 1, dst], f2r.at[b - 1, src], zdev(dst)
        )

    for b in range(1, ib):
        def f2_start(i):
            dst = wrap(p + 1 + i)

            @pl.when(bit_of(dst, b) == 1)
            def _():
                f2(b, dst, p).start()

        loop(n - 1, f2_start)

        @pl.when(bit_of(p, b) == 1)
        def _():
            LS[p, lev(b), :] = IS[b - 1, lax.div(p, 2 ** (b + 1))]

    def masked_sum(ref, count, me, m):
        out = jnp.zeros((DK, DK), F32)
        for i in range(count):
            cond = (
                (bit_of(me, m) == 1)
                & (lax.div(me, 2 ** (m + 1)) == i >> (m + 1))
                & ((i >> m) % 2 == 0)
            )
            out = out + jnp.where(cond, ref[i].astype(F32), 0.0)
        return out

    def f3(way, m, s, head):
        dst = wrap(p + 1) if way == 0 else wrap(p - 1)
        slot = LS.at[head, lev(ib + m), :]
        return rc(slot, slot, f3s.at[way, m, s], f3r.at[way, m, s], zdev(dst))

    hops = (half, half - 1)

    def on_bit(m, body):
        @pl.when(bit_of(g, m) == 1)
        def _():
            body()

    def f3_step(m, s):
        for way in range(2):
            if s > 0 and s - 1 < hops[way]:
                head = wrap(p - s) if way == 0 else wrap(p + s)
                f3(way, m, s - 1, head).wait_recv()
            if s < hops[way]:
                head = wrap(p - s) if way == 0 else wrap(p + s)
                f3(way, m, s, head).start()

    def fy_wait(j):
        src = lax.rem(y + 1 + j, nlo)
        fy(j, src).wait_recv()

    loop(nlo - 1, fy_wait)
    for m in range(lob):
        on_bit(m, lambda: LS.__setitem__((p, lev(ib + m)), masked_sum(YR, nlo, y, m).astype(BF16)))
    parts = [YR[i].astype(F32) for i in range(nlo)]
    YT[...] = sum(parts[1:], parts[0]).astype(BF16)
    for m in range(lob):
        on_bit(m, lambda: f3_step(m, 0))

    def fx(dst, src):
        return rc(YT, XR.at[src], fxs.at[dst], fxr.at[src], xdev(dst))

    def fx_start(j):
        @pl.when(x + 1 + j < nhi)
        def _():
            fx(x + 1 + j, x).start()

    def fx_wait(j):
        @pl.when(j < x)
        def _():
            fx(j, j).wait_recv()

    loop(nhi - 1, fx_start)
    loop(nhi - 1, fx_wait)
    for m in range(hib):
        on_bit(lob + m, lambda: LS.__setitem__((p, lev(ib + lob + m)), masked_sum(XR, nhi, x, m).astype(BF16)))
    for m in range(hib):
        on_bit(lob + m, lambda: f3_step(lob + m, 0))

    @pl.when(bit_of(p, 0) == 1)
    def _():
        fl1_copy.wait_recv()

    def b2(b, dst, src):
        return rc(AD.at[dst, b], AI.at[b - 1, src], b2s.at[b - 1, dst], b2r.at[b - 1, src], zdev(dst))

    def finish(h):
        inter = nn(QC[h], LS[h])
        error = (COEF[0] * IN[h] + inter - Y[h].astype(F32)).astype(BF16)
        ER[h] = error
        adjoint = tn(error, QC[h]).astype(BF16)
        for b in range(nb):
            AD[h, b] = adjoint[:, b * DK : (b + 1) * DK]

    def far(h):
        for b in range(1, ib):
            @pl.when(bit_of(p, b) == 1)
            def _():
                f2(b, p, h).wait_recv()
        finish(h)

    def far_send(h):
        for b in range(1, ib):
            @pl.when(bit_of(p, b) == 1)
            def _():
                b2(b, h, p).start()

    finish(p)
    for b in range(1, ib):
        @pl.when(bit_of(p, b) == 1)
        def _():
            AI[b - 1, p] = AD[p, b]

    for s in range(1, half + 1):
        for m in range(ob):
            on_bit(m, lambda: f3_step(m, s))
        heads = [wrap(p - s)] + ([wrap(p + s)] if s < half else [])
        def both(i):
            h = wrap(p - s + 2 * s * i)
            far(h)
        loop(len(heads), both)
        for h in heads:
            far_send(h)

    def b3(way, m, s):
        head = wrap(p + half - s) if way == 0 else wrap(p - (half - 1) + s)
        dst = wrap(p + 1) if way == 0 else wrap(p - 1)
        return rc(
            AD.at[head, ib + m], RP.at[way, m, s], b3s.at[way, m, s], b3r.at[way, m, s], zdev(dst)
        )

    def b3_step(m, s):
        for way in range(2):
            if s < hops[way]:
                if s > 0:
                    b3(way, m, s - 1).wait_recv()
                    head = wrap(p + half - s) if way == 0 else wrap(p - (half - 1) + s)
                    AD[head, ib + m] = (
                        AD[head, ib + m].astype(F32) + RP[way, m, s - 1].astype(F32)
                    ).astype(BF16)
                b3(way, m, s).start()

    for m in range(ob):
        on_bit(m, lambda: b3_step(m, 0))

    bl1_copy = rc(AD.at[:, 0], AL1, bl1.at[0], bl1.at[1], zdev(wrap(p - 1)))

    @pl.when(bit_of(p, 0) == 1)
    def _():
        bl1_copy.start()

    def heavy(h):
        error = ER[h]
        error32 = error.astype(F32)
        query = Q[h]
        query32 = query.astype(F32)
        key = K[h]
        intra_error = (COEF[0] * error32).astype(BF16)
        raw = nt(intra_error, V[h]) * gamma
        score_grad = jnp.where(lower(), raw, 0.0).astype(BF16)
        back = nt(error, LS[h])
        grad = nn(score_grad, key)
        GACC[0] += error32 * IN[h]
        for b in range(nb):
            piece = back[:, b * DK : (b + 1) * DK]
            grad = grad + COEF[b + 1] * piece
            GACC[b + 1] += query32 * piece
        OQ[h] = grad.astype(BF16)
        GK[h] = tn(score_grad, query)
        GV[h] = tn(SC[h], intra_error)

    per_step = n // (half + 1) if half > 1 else 1
    done = 0

    def some(count):
        nonlocal done
        count = min(count, n - done)
        first = done
        if count > 0:
            loop(count, lambda i: heavy(first + i))
        done = first + count

    for s in range(1, half):
        some(per_step)
        for m in range(ob):
            on_bit(m, lambda: b3_step(m, s))
    some(per_step)

    def own(m):
        value = AD[p, ib + m].astype(F32) + RP[0, m, hops[0] - 1].astype(F32)
        if hops[1] > 0:
            value = value + RP[1, m, hops[1] - 1].astype(F32)
        return value

    for m in reversed(range(ob)):
        def own_wait():
            for way in range(2):
                if hops[way] > 0:
                    b3(way, m, hops[way] - 1).wait_recv()
            if m >= lob:
                BXS[m - lob] = own(m).astype(BF16)
        on_bit(m, own_wait)

    def bx(m, dst, src):
        return rc(BXS.at[m], BXR.at[src], bxs.at[dst], bxr.at[src], xdev(dst))

    def top_bit(a, b, m):
        return (lax.div(a, 2 ** (m + 1)) == lax.div(b, 2 ** (m + 1))) & (
            lax.div(a, 2**m) != lax.div(b, 2**m)
        )

    for j in range(nhi - 1):
        for m in range(hib):
            @pl.when((j < x) & top_bit(x, jnp.int32(j), m))
            def _():
                bx(m, j, x).start()

    some(1)

    for j in range(1, nhi):
        @pl.when(j > x)
        def _():
            bx(0, 0, j).wait_recv()

    outer = jnp.zeros((DK, DK), F32)
    for j in range(1, nhi):
        outer = outer + jnp.where(j > x, BXR[j].astype(F32), 0.0)
    BYS[0] = outer.astype(BF16)
    for m in range(lob):
        @pl.when(bit_of(y, m) == 1)
        def _():
            BYS[m + 1] = (outer + own(m)).astype(BF16)

    def by(kind, dst, src):
        return rc(BYS.at[kind], BYR.at[src], bys.at[dst], byr.at[src], ydev(dst))

    for j in range(nlo):
        @pl.when(j > y)
        def _():
            by(0, j, y).start()
        for m in range(lob):
            @pl.when((j < y) & top_bit(y, jnp.int32(j), m))
            def _():
                by(m + 1, j, y).start()

    some(1)

    for b in range(1, ib):
        def b2_wait(i):
            src = wrap(p + 1 + i)

            @pl.when(bit_of(src, b) == 1)
            def _():
                b2(b, src, src).wait_recv()

        loop(n - 1, b2_wait)

    for j in range(nlo):
        @pl.when(j != y)
        def _():
            by(0, j, j).wait_recv()
    for j in range(nlo):
        outer = outer + jnp.where(j != y, BYR[j].astype(F32), 0.0)
    nodes = {}
    for b in range(1, ib):
        for node in range(n // 2 ** (b + 1)):
            first = node * 2 ** (b + 1) + 2**b
            members = [AI[b - 1, c].astype(F32) for c in range(first, first + 2**b)]
            nodes[b, node] = sum(members[1:], members[0])
    for dst in range(n):
        value = outer
        for b in range(1, ib):
            if (dst >> b) % 2 == 0:
                value = value + nodes[b, dst >> (b + 1)]
        DS[dst] = value.astype(BF16)
    BA[p] = DS[p]

    def b4(dst, src):
        return rc(DS.at[dst], BA.at[src], b4s.at[dst], b4r.at[src], zdev(dst))

    loop(half, lambda i: b4(wrap(p + half + i), p).start())
    loop(half - 1, lambda i: b4(wrap(p + 1 + i), p).start())
    some(n)

    row = lax.broadcasted_iota(jnp.int32, (nb + 1, rows), 0)
    ones = jnp.ones((nb + 1, DK), F32)
    mine = jnp.zeros((nb + 1, rows), F32)
    for num in range(nb + 1):
        sums = lax.dot_general(
            ones, GACC[num], (((1,), (1,)), ((), ())),
            precision=lax.Precision.HIGHEST, preferred_element_type=F32,
        )
        mine = jnp.where(row == num, sums * scales[num], mine)
    GLP[...] = mine
    loop(n, lambda h: out_copy(0, h).start())
    if nhead == 2:
        glx_copy = rc(GLP, GLR, glx.at[0], glx.at[1], (1 - hd, g, p))
        glx_copy.start()

    @pl.when(low0)
    def _():
        bl1_copy.wait_recv()

    def last(i):
        h = wrap(p + i)

        @pl.when(i > 0)
        def _():
            b4(h, h).wait_recv()
        adjoint = BA[h].astype(F32) + jnp.where(low0, AL1[h].astype(F32), 0.0)
        low = adjoint.astype(BF16)
        OK[h] = (GK[h] + nn(V[h], low)).astype(BF16)
        OV[h] = (GV[h] + nt(K[h], low)).astype(BF16)
        out_copy(1, h).start()
        out_copy(2, h).start()

    loop(n, last)

    if nhead == 2:
        glx_copy.wait_recv()
        glx_copy.wait_send()
        GLP[...] = GLP[...] + GLR[...]
    gl_copy = pltpu.make_async_copy(GLP, gl_hbm, gl_sem)
    gl_copy.start()

    loop(n - 1, lambda i: f1(wrap(p + 1 + i), p).wait_send())

    @pl.when(low0)
    def _():
        fl1_copy.wait_send()

    @pl.when(bit_of(p, 0) == 1)
    def _():
        bl1_copy.wait_send()

    loop(nlo - 1, lambda j: fy(j, y).wait_send())

    def fx_sent(j):
        @pl.when(x + 1 + j < nhi)
        def _():
            fx(x + 1 + j, x).wait_send()

    loop(nhi - 1, fx_sent)
    for b in range(1, ib):
        def sent(i):
            dst = wrap(p + 1 + i)

            @pl.when(bit_of(dst, b) == 1)
            def _():
                f2(b, dst, p).wait_send()

            @pl.when(bit_of(p, b) == 1)
            def _():
                b2(b, dst, p).wait_send()

        loop(n - 1, sent)
    for m in range(ob):
        def chain_sent():
            for way in range(2):
                for s in range(hops[way]):
                    f3(way, m, s, wrap(p - s) if way == 0 else wrap(p + s)).wait_send()
                    b3(way, m, s).wait_send()
        on_bit(m, chain_sent)
    for j in range(nhi - 1):
        @pl.when(j < x)
        def _():
            bx(0, j, x).wait_send()
    for j in range(nlo):
        @pl.when(j != y)
        def _():
            by(0, j, y).wait_send()
    loop(n - 1, lambda i: b4(wrap(p + 1 + i), p).wait_send())

    def written(h):
        for a in range(3):
            out_copy(a, h).wait()

    loop(n, written)
    gl_copy.wait()


def on_device(queries, key_rows, value_rows, teacher_out, level_weights):
    rows, width = queries.shape
    heads = width // DK
    n = lax.axis_size("inner")
    outer_count = lax.axis_size("outer")
    nhead = lax.axis_size("head")
    assert heads == n
    ib = n.bit_length() - 1
    ob = outer_count.bit_length() - 1
    lob = ob // 2
    hib = ob - lob
    nlo, nhi = 2**lob, 2**hib
    nb = ib + ob
    levels = level_weights.shape[0]
    assert levels == nb + 1
    gamma = DK ** (-0.5)
    scales = [rows ** (-0.5)] + [gamma * (rows * 2 ** (num - 1)) ** (-0.5) for num in range(1, levels)]
    dims = (n, nlo, nhi, nhead, ib, lob, hib, rows, tuple(scales), gamma)
    half = n // 2
    ibx = max(ib - 1, 1)
    any_spec = pl.BlockSpec(memory_space=pl.ANY)
    dma = pltpu.SemaphoreType.DMA

    def low(*shape):
        return pltpu.VMEM(shape, BF16)

    def wide(*shape):
        return pltpu.VMEM(shape, F32)

    sq = (DK, DK)
    scratch = [
        low(n, rows, DK), low(n, rows, DK), low(n, rows, DK), low(n, rows, DK), low(levels, rows),
        low(n, *sq), low(n, *sq), low(n, nb * DK, DK), low(ibx, max(n // 4, 1), *sq),
        low(*sq), low(nlo, *sq), low(*sq), low(nhi, *sq),
        wide(levels, rows, DK), low(n, rows, nb * DK), low(n, rows, rows), wide(n, rows, DK),
        low(n, rows, DK), low(n, nb, *sq),
        low(n, *sq), low(ibx, n, *sq), low(2, ob, half, *sq), low(hib, *sq), low(nhi, *sq),
        low(lob + 1, *sq), low(nlo, *sq), low(n, *sq), low(n, *sq),
        wide(n, rows, DK), wide(n, rows, DK), low(n, rows, DK), low(n, rows, DK), low(n, rows, DK),
        wide(levels, rows, DK), wide(levels, rows), wide(levels, rows),
        dma((4, n)), dma(()), dma((3, n)), dma(()),
        dma((n,)), dma((n,)), dma((2,)), dma((ibx, n)), dma((ibx, n)),
        dma((nlo,)), dma((nlo,)), dma((nhi,)), dma((nhi,)), dma((2, ob, half)), dma((2, ob, half)),
        dma((2,)), dma((ibx, n)), dma((ibx, n)), dma((2, ob, half)), dma((2, ob, half)),
        dma((nhi,)), dma((nhi,)), dma((nlo,)), dma((nlo,)), dma((n,)), dma((n,)), dma((2,)),
    ]
    big = jax.ShapeDtypeStruct((rows, width), BF16)
    return pl.pallas_call(
        functools.partial(kernel, dims),
        out_shape=(big, big, big, jax.ShapeDtypeStruct((levels, rows), F32)),
        in_specs=[any_spec] * 5,
        out_specs=[any_spec] * 4,
        scratch_shapes=scratch,
        compiler_params=pltpu.CompilerParams(
            collective_id=0, has_side_effects=True, vmem_limit_bytes=60 * 2**20
        ),
        name="log_linear",
    )(queries, key_rows, value_rows, teacher_out, level_weights)


def solution(mesh):
    tokens = P(("outer", "inner"), "head")
    per_token = P(None, ("outer", "inner"))
    return jax.shard_map(
        on_device,
        mesh=mesh,
        in_specs=(tokens, tokens, tokens, tokens, per_token),
        out_specs=(tokens, tokens, tokens, per_token),
        check_vma=False,
    )
```

```python
import functools

import jax
import jax.numpy as jnp
from jax import lax
from jax.experimental import pallas as pl
from jax.experimental.pallas import tpu as pltpu
from jax.sharding import PartitionSpec as P

DK = 128
MESH = pl.DeviceIdType.MESH
F32 = jnp.float32
BF16 = jnp.bfloat16


def nn(a, b):
    return lax.dot_general(a, b, (((1,), (0,)), ((), ())), preferred_element_type=F32)


def nt(a, b):
    return lax.dot_general(a, b, (((1,), (1,)), ((), ())), preferred_element_type=F32)


def tn(a, b):
    return lax.dot_general(a, b, (((0,), (0,)), ((), ())), preferred_element_type=F32)


def bit_of(number, position):
    return lax.rem(lax.div(number, 2**position), 2)


def kernel(
    dims,
    q_hbm, k_hbm, v_hbm, y_hbm, w_hbm,
    gq_hbm, gk_hbm, gv_hbm, gl_hbm, ba_hbm,
    Q, K, V, Y, W, BS, FR, LS, IS, TOT, YR, YT, XR, COEF, QC, SC, IN, ER, AD,
    AL1, AI, RP, BXS, BXR, BYS, BYR, DS, BA, DA, OQ, OK, OV, GACC, GLP, GLR,
    in_sem, w_sem, out_sem, gl_sem, ba_sem,
    f1s, f1r, fl1, f2s, f2r, fys, fyr, fxs, fxr, f3s, f3r,
    bl1, b2s, b2r, b3s, b3r, bxs, bxr, bys, byr, b4s, b4r, glx,
):
    n, nlo, nhi, nhead, ib, lob, hib, rows, scales, gamma = dims
    ob = lob + hib
    nb = ib + ob
    half = n // 2
    p = lax.axis_index("inner")
    g = lax.axis_index("outer")
    hd = lax.axis_index("head")
    x = lax.div(g, nlo)
    y = lax.rem(g, nlo)

    def zdev(r):
        return (hd, g, r)

    def odev(o):
        return (hd, o, p)

    def ydev(yy):
        return odev(x * nlo + yy)

    def xdev(xx):
        return odev(xx * nlo + y)

    def wrap(i):
        return lax.rem(i + 2 * n, n)

    def loop(count, body, unroll=1):
        def step(i, c):
            body(i)
            return c
        lax.fori_loop(0, count, step, 0, unroll=unroll)

    def rc(src, dst, ss, rs, dev):
        return pltpu.make_async_remote_copy(
            src_ref=src, dst_ref=dst, send_sem=ss, recv_sem=rs, device_id=dev, device_id_type=MESH
        )

    def cols(h):
        return pl.ds(pl.multiple_of(h * DK, DK), DK)

    def lev(b):
        return pl.ds(b * DK, DK)

    def in_copy(a, h):
        hbm, vm = ((k_hbm, K), (v_hbm, V), (q_hbm, Q), (y_hbm, Y))[a]
        return pltpu.make_async_copy(hbm.at[:, cols(h)], vm.at[h], in_sem.at[a, h])

    def out_copy(a, h):
        hbm, vm = ((gq_hbm, OQ), (gk_hbm, OK), (gv_hbm, OV))[a]
        return pltpu.make_async_copy(vm.at[h], hbm.at[:, cols(h)], out_sem.at[a, h])

    def start_kv(h):
        in_copy(0, h).start()
        in_copy(1, h).start()

    def start_qy(h):
        in_copy(2, h).start()
        in_copy(3, h).start()

    loop(n, start_kv)
    w_copy = pltpu.make_async_copy(w_hbm, W, w_sem)
    w_copy.start()
    loop(n, start_qy)

    barrier = pltpu.get_barrier_semaphore()

    def greet(dev):
        pl.semaphore_signal(barrier, inc=1, device_id=dev, device_id_type=MESH)

    loop(n - 1, lambda i: greet(zdev(wrap(p + 1 + i))))
    loop(nlo - 1, lambda i: greet(ydev(lax.rem(y + 1 + i, nlo))))
    loop(nhi - 1, lambda i: greet(xdev(lax.rem(x + 1 + i, nhi))))
    if nhead == 2:
        greet((1 - hd, g, p))

    def state(h):
        in_copy(0, h).wait()
        in_copy(1, h).wait()
        BS[h] = tn(K[h], V[h]).astype(BF16)


    def f1(h, src):
        return rc(BS.at[h], FR.at[src], f1s.at[h], f1r.at[src], zdev(h))

    def nth(i):
        near = half - lax.div(i + 1, 2)
        return wrap(p + near * (1 - 2 * lax.rem(i, 2)))

    state(nth(0))
    if n > 2:
        state(nth(1))
    pl.semaphore_wait(barrier, (n - 1) + (nlo - 1) + (nhi - 1) + (nhead - 1))

    def f1_start(i):
        f1(nth(i), p).start()

        @pl.when(i + 2 < n)
        def _():
            state(nth(i + 2))

    loop(n - 1, f1_start)
    if n == 2:
        state(p)
    fl1_copy = rc(BS, LS.at[:, lev(0), :], fl1.at[0], fl1.at[1], zdev(wrap(p + 1)))
    low0 = bit_of(p, 0) == 0

    @pl.when(low0)
    def _():
        fl1_copy.start()

    FR[p] = BS[p]

    w_copy.wait()
    for b in range(nb):
        bit = bit_of(p, b) if b < ib else bit_of(g, b - ib)

        @pl.when(bit == 0)
        def _():
            LS[:, lev(b), :] = jnp.zeros((n, DK, DK), BF16)

    weights = W[...]
    pick = lax.broadcasted_iota(jnp.int32, (nb + 1, DK), 0)
    for num in range(nb + 1):
        COEF[num] = tn(weights, jnp.where(pick == num, 1.0, 0.0).astype(BF16)) * scales[num]
    GACC[...] = jnp.zeros_like(GACC)

    def lower():
        return lax.broadcasted_iota(jnp.int32, (rows, rows), 0) >= lax.broadcasted_iota(
            jnp.int32, (rows, rows), 1
        )

    def ahead(h):
        in_copy(2, h).wait()
        in_copy(3, h).wait()
        query = Q[h]
        scores = nt(query, K[h]) * gamma
        kept = jnp.where(lower(), scores, 0.0).astype(BF16)
        SC[h] = kept
        IN[h] = nn(kept, V[h])
        query32 = query.astype(F32)
        for b in range(nb):
            QC[h, :, lev(b)] = (query32 * COEF[b + 1]).astype(BF16)

    loop(n, ahead)

    def f1_wait(i):
        src = wrap(p + 1 + i)
        f1(src, src).wait_recv()

    loop(n - 1, f1_wait)
    states = [FR[i].astype(F32) for i in range(n)]
    total = sum(states[1:], states[0])
    TOT[...] = total.astype(BF16)
    for b in range(1, ib):
        for node in range(n // 2 ** (b + 1)):
            first = node * 2 ** (b + 1)
            members = states[first : first + 2**b]
            IS[b - 1, node] = sum(members[1:], members[0]).astype(BF16)
    YR[y] = TOT[...]

    def fy(j, src):
        return rc(TOT, YR.at[src], fys.at[j], fyr.at[src], ydev(lax.rem(y + 1 + j, nlo)))

    loop(nlo - 1, lambda j: fy(j, y).start())

    def f2(b, dst, src):
        node = lax.div(dst, 2 ** (b + 1))
        return rc(
            IS.at[b - 1, node], LS.at[src, lev(b), :], f2s.at[b - 1, dst], f2r.at[b - 1, src], zdev(dst)
        )

    for b in range(1, ib):
        def f2_start(i):
            dst = wrap(p + 1 + i)

            @pl.when(bit_of(dst, b) == 1)
            def _():
                f2(b, dst, p).start()

        loop(n - 1, f2_start)

        @pl.when(bit_of(p, b) == 1)
        def _():
            LS[p, lev(b), :] = IS[b - 1, lax.div(p, 2 ** (b + 1))]

    def masked_sum(ref, count, me, m):
        out = jnp.zeros((DK, DK), F32)
        for i in range(count):
            cond = (
                (bit_of(me, m) == 1)
                & (lax.div(me, 2 ** (m + 1)) == i >> (m + 1))
                & ((i >> m) % 2 == 0)
            )
            out = out + jnp.where(cond, ref[i].astype(F32), 0.0)
        return out

    def f3(way, m, s, head):
        dst = wrap(p + 1) if way == 0 else wrap(p - 1)
        rows_here = part(way) if s == half - 1 else (0, DK)
        slot = LS.at[head, pl.ds((ib + m) * DK + rows_here[0], rows_here[1]), :]
        return rc(slot, slot, f3s.at[way, m, s], f3r.at[way, m, s], zdev(dst))

    hops = half

    def part(way):
        return (way * (DK // 2), DK // 2)

    def on_bit(m, body):
        @pl.when(bit_of(g, m) == 1)
        def _():
            body()

    def f3_step(m, s):
        for way in range(2):
            if s > 0:
                head = wrap(p - s) if way == 0 else wrap(p + s)
                f3(way, m, s - 1, head).wait_recv()
            if s < hops:
                head = wrap(p - s) if way == 0 else wrap(p + s)
                f3(way, m, s, head).start()

    def fy_wait(j):
        src = lax.rem(y + 1 + j, nlo)
        fy(j, src).wait_recv()

    loop(nlo - 1, fy_wait)
    for m in range(lob):
        on_bit(m, lambda: LS.__setitem__((p, lev(ib + m)), masked_sum(YR, nlo, y, m).astype(BF16)))
    parts = [YR[i].astype(F32) for i in range(nlo)]
    YT[...] = sum(parts[1:], parts[0]).astype(BF16)
    for m in range(lob):
        on_bit(m, lambda: f3_step(m, 0))

    def fx(dst, src):
        return rc(YT, XR.at[src], fxs.at[dst], fxr.at[src], xdev(dst))

    def fx_start(j):
        @pl.when(x + 1 + j < nhi)
        def _():
            fx(x + 1 + j, x).start()

    def fx_wait(j):
        @pl.when(j < x)
        def _():
            fx(j, j).wait_recv()

    loop(nhi - 1, fx_start)
    for m in range(lob):
        on_bit(m, lambda: f3_step(m, 1))
    loop(nhi - 1, fx_wait)
    for m in range(hib):
        on_bit(lob + m, lambda: LS.__setitem__((p, lev(ib + lob + m)), masked_sum(XR, nhi, x, m).astype(BF16)))
    for m in range(hib):
        on_bit(lob + m, lambda: f3_step(lob + m, 0))

    @pl.when(bit_of(p, 0) == 1)
    def _():
        fl1_copy.wait_recv()

    def b2(b, dst, src):
        return rc(AD.at[dst, b], AI.at[b - 1, src], b2s.at[b - 1, dst], b2r.at[b - 1, src], zdev(dst))

    def finish(h):
        inter = nn(QC[h], LS[h])
        error = (COEF[0] * IN[h] + inter - Y[h].astype(F32)).astype(BF16)
        ER[h] = error
        adjoint = tn(error, QC[h]).astype(BF16)
        for b in range(nb):
            AD[h, b] = adjoint[:, b * DK : (b + 1) * DK]

    def far(h):
        for b in range(1, ib):
            @pl.when(bit_of(p, b) == 1)
            def _():
                f2(b, p, h).wait_recv()
        finish(h)

    finish(p)
    for b in range(1, ib):
        @pl.when(bit_of(p, b) == 1)
        def _():
            AI[b - 1, p] = AD[p, b]

    for s in range(1, half + 1):
        if s < half:
            for m in range(lob):
                on_bit(m, lambda: f3_step(m, s + 1))
        for m in range(lob, ob):
            on_bit(m, lambda: f3_step(m, s))
        heads = [wrap(p - s)] + ([wrap(p + s)] if s < half else [])
        def both(i):
            h = wrap(p - s + 2 * s * i)
            far(h)
        loop(len(heads), both)

    def b3(way, m, s):
        dst = wrap(p + 1) if way == 0 else wrap(p - 1)
        some_rows = pl.ds(*(part(way) if s == 0 else (0, DK)))
        return rc(
            AD.at[chained(way, s), ib + m, some_rows], RP.at[way, m, s, some_rows],
            b3s.at[way, m, s], b3r.at[way, m, s], zdev(dst),
        )

    def chained(way, s):
        return wrap(p + half - s) if way == 0 else wrap(p - half + s)

    def b3_step(m, s):
        for way in range(2):
            if s > 0:
                b3(way, m, s - 1).wait_recv()
                some_rows = pl.ds(*(part(way) if s == 1 else (0, DK)))
                head = chained(way, s)
                AD[head, ib + m, some_rows] = (
                    AD[head, ib + m, some_rows].astype(F32) + RP[way, m, s - 1, some_rows].astype(F32)
                ).astype(BF16)
            b3(way, m, s).start()

    for m in reversed(range(ob)):
        on_bit(m, lambda: b3_step(m, 0))

    bl1_copy = rc(AD.at[:, 0], AL1, bl1.at[0], bl1.at[1], zdev(wrap(p - 1)))

    def heavy(h):
        error = ER[h]
        error32 = error.astype(F32)
        query = Q[h]
        query32 = query.astype(F32)
        key = K[h]
        intra_error = (COEF[0] * error32).astype(BF16)
        raw = nt(intra_error, V[h]) * gamma
        score_grad = jnp.where(lower(), raw, 0.0).astype(BF16)
        back = nt(error, LS[h])
        grad = nn(score_grad, key)
        GACC[0] += error32 * IN[h]
        for b in range(nb):
            piece = back[:, b * DK : (b + 1) * DK]
            grad = grad + COEF[b + 1] * piece
            GACC[b + 1] += query32 * piece
        OQ[h] = grad.astype(BF16)
        OK[h] = tn(score_grad, query).astype(BF16)
        OV[h] = tn(SC[h], intra_error).astype(BF16)

    per_step = n // (half + 1) if half > 1 else 1
    done = 0

    def some(count):
        nonlocal done
        count = min(count, n - done)
        first = done
        if count > 0:
            loop(count, lambda i: heavy(first + i))
        done = first + count

    for s in range(1, half):
        some(per_step)
        for m in reversed(range(ob)):
            on_bit(m, lambda: b3_step(m, s))

    for b in reversed(range(1, ib)):
        @pl.when(bit_of(p, b) == 1)
        def _():
            loop(n - 1, lambda i: b2(b, wrap(p + 1 + i), p).start())

    @pl.when(bit_of(p, 0) == 1)
    def _():
        bl1_copy.start()

    some(per_step)

    def own(m):
        first, second = RP[0, m, half - 1].astype(F32), RP[1, m, half - 1].astype(F32)
        if half == 1:
            top = lax.broadcasted_iota(jnp.int32, (DK, DK), 0) < DK // 2
            return AD[p, ib + m].astype(F32) + jnp.where(top, first, second)
        return AD[p, ib + m].astype(F32) + first + second

    def own_wait(m):
        for way in range(2):
            b3(way, m, half - 1).wait_recv()
        if m >= lob:
            BXS[m - lob] = own(m).astype(BF16)

    for m in reversed(range(lob, ob)):
        on_bit(m, lambda: own_wait(m))

    def bx(m, dst, src):
        return rc(BXS.at[m], BXR.at[src], bxs.at[dst], bxr.at[src], xdev(dst))

    def top_bit(a, b, m):
        return (lax.div(a, 2 ** (m + 1)) == lax.div(b, 2 ** (m + 1))) & (
            lax.div(a, 2**m) != lax.div(b, 2**m)
        )

    for j in range(nhi - 1):
        for m in range(hib):
            @pl.when((j < x) & top_bit(x, jnp.int32(j), m))
            def _():
                bx(m, j, x).start()

    for m in range(lob):
        on_bit(m, lambda: own_wait(m))
    some(1)

    for j in range(1, nhi):
        @pl.when(j > x)
        def _():
            bx(0, 0, j).wait_recv()

    outer = jnp.zeros((DK, DK), F32)
    for j in range(1, nhi):
        outer = outer + jnp.where(j > x, BXR[j].astype(F32), 0.0)
    BYS[0] = outer.astype(BF16)
    for m in range(lob):
        @pl.when(bit_of(y, m) == 1)
        def _():
            BYS[m + 1] = (outer + own(m)).astype(BF16)

    def by(kind, dst, src):
        return rc(BYS.at[kind], BYR.at[src], bys.at[dst], byr.at[src], ydev(dst))

    for j in range(nlo):
        @pl.when(j > y)
        def _():
            by(0, j, y).start()
        for m in range(lob):
            @pl.when((j < y) & top_bit(y, jnp.int32(j), m))
            def _():
                by(m + 1, j, y).start()

    some(1)

    for b in range(1, ib):
        def b2_wait(i):
            src = wrap(p + 1 + i)

            @pl.when(bit_of(src, b) == 1)
            def _():
                b2(b, src, src).wait_recv()

        loop(n - 1, b2_wait)

    for j in range(nlo):
        @pl.when(j != y)
        def _():
            by(0, j, j).wait_recv()
    for j in range(nlo):
        outer = outer + jnp.where(j != y, BYR[j].astype(F32), 0.0)
    nodes = {}
    for b in range(1, ib):
        for node in range(n // 2 ** (b + 1)):
            first = node * 2 ** (b + 1) + 2**b
            members = [AI[b - 1, c].astype(F32) for c in range(first, first + 2**b)]
            nodes[b, node] = sum(members[1:], members[0])
    for dst in range(n):
        value = outer
        for b in range(1, ib):
            if (dst >> b) % 2 == 0:
                value = value + nodes[b, dst >> (b + 1)]
        DS[dst] = value.astype(BF16)
    BA[p] = DS[p]

    def b4(dst, src):
        return rc(DS.at[dst], BA.at[src], b4s.at[dst], b4r.at[src], zdev(dst))

    loop(half, lambda i: b4(wrap(p + half + i), p).start())
    loop(half - 1, lambda i: b4(wrap(p + 1 + i), p).start())
    some(n)

    row = lax.broadcasted_iota(jnp.int32, (nb + 1, rows), 0)
    ones = jnp.ones((nb + 1, DK), F32)
    mine = jnp.zeros((nb + 1, rows), F32)
    for num in range(nb + 1):
        sums = lax.dot_general(
            ones, GACC[num], (((1,), (1,)), ((), ())),
            precision=lax.Precision.HIGHEST, preferred_element_type=F32,
        )
        mine = jnp.where(row == num, sums * scales[num], mine)
    GLP[...] = mine

    def write(h):
        for a in range(3):
            out_copy(a, h).start()

    loop(n, write)
    if nhead == 2:
        glx_copy = rc(GLP, GLR, glx.at[0], glx.at[1], (1 - hd, g, p))
        glx_copy.start()

    @pl.when(low0)
    def _():
        bl1_copy.wait_recv()

    def last(i):
        h = wrap(p + i)

        @pl.when(i > 0)
        def _():
            b4(h, h).wait_recv()
        adjoint = BA[h].astype(F32) + jnp.where(low0, AL1[h].astype(F32), 0.0)
        DA[h] = adjoint.astype(BF16)

    loop(n, last)
    ba_copy = pltpu.make_async_copy(DA, ba_hbm, ba_sem)
    ba_copy.start()

    if nhead == 2:
        glx_copy.wait_recv()
        glx_copy.wait_send()
        GLP[...] = GLP[...] + GLR[...]
    gl_copy = pltpu.make_async_copy(GLP, gl_hbm, gl_sem)
    gl_copy.start()

    loop(n - 1, lambda i: f1(wrap(p + 1 + i), p).wait_send())

    @pl.when(low0)
    def _():
        fl1_copy.wait_send()

    @pl.when(bit_of(p, 0) == 1)
    def _():
        bl1_copy.wait_send()

    loop(nlo - 1, lambda j: fy(j, y).wait_send())

    def fx_sent(j):
        @pl.when(x + 1 + j < nhi)
        def _():
            fx(x + 1 + j, x).wait_send()

    loop(nhi - 1, fx_sent)
    for b in range(1, ib):
        def sent(i):
            dst = wrap(p + 1 + i)

            @pl.when(bit_of(dst, b) == 1)
            def _():
                f2(b, dst, p).wait_send()

            @pl.when(bit_of(p, b) == 1)
            def _():
                b2(b, dst, p).wait_send()

        loop(n - 1, sent)
    for m in range(ob):
        def chain_sent():
            for way in range(2):
                for s in range(hops):
                    f3(way, m, s, wrap(p - s) if way == 0 else wrap(p + s)).wait_send()
                    b3(way, m, s).wait_send()
        on_bit(m, chain_sent)
    for j in range(nhi - 1):
        @pl.when(j < x)
        def _():
            bx(0, j, x).wait_send()
    for j in range(nlo):
        @pl.when(j != y)
        def _():
            by(0, j, y).wait_send()
    loop(n - 1, lambda i: b4(wrap(p + 1 + i), p).wait_send())

    def written(h):
        for a in range(3):
            out_copy(a, h).wait()

    loop(n, written)
    gl_copy.wait()
    ba_copy.wait()


def finish_kernel(
    n, pq_hbm, pk_hbm, pv_hbm, k_hbm, v_hbm, pl_hbm, a_hbm, gq_hbm, gk_hbm, gv_hbm, gl_hbm,
    GQ, PK, PV, K, V, GL, A, GK, GV, in_sem, out_sem, a_sem, l_sem,
):
    def loop(body):
        def step(i, c):
            body(i)
            return c
        lax.fori_loop(0, n, step, 0)

    def cols(h):
        return pl.ds(pl.multiple_of(h * DK, DK), DK)

    ins = ((pq_hbm, GQ), (pk_hbm, PK), (pv_hbm, PV), (k_hbm, K), (v_hbm, V))
    outs = ((gq_hbm, GQ), (gk_hbm, GK), (gv_hbm, GV))

    def in_copy(a, h):
        return pltpu.make_async_copy(ins[a][0].at[:, cols(h)], ins[a][1].at[h], in_sem.at[a, h])

    def out_copy(a, h):
        return pltpu.make_async_copy(outs[a][1].at[h], outs[a][0].at[:, cols(h)], out_sem.at[a, h])

    a_copy = pltpu.make_async_copy(a_hbm, A, a_sem)
    a_copy.start()
    l_copy = pltpu.make_async_copy(pl_hbm, GL, l_sem.at[0])
    l_copy.start()

    def start(h):
        for a in (4, 1, 3, 2, 0):
            in_copy(a, h).start()

    loop(start)
    l_copy.wait()
    l_out = pltpu.make_async_copy(GL, gl_hbm, l_sem.at[1])
    l_out.start()
    a_copy.wait()

    def one(h):
        for a in (4, 1, 3, 2, 0):
            in_copy(a, h).wait()
        out_copy(0, h).start()
        adjoint = A[h]
        GK[h] = (PK[h].astype(F32) + nn(V[h], adjoint)).astype(BF16)
        GV[h] = (PV[h].astype(F32) + nt(K[h], adjoint)).astype(BF16)
        out_copy(1, h).start()
        out_copy(2, h).start()

    loop(one)

    def done(h):
        for a in range(3):
            out_copy(a, h).wait()

    loop(done)
    l_out.wait()


def on_device(queries, key_rows, value_rows, teacher_out, level_weights):
    rows, width = queries.shape
    heads = width // DK
    n = lax.axis_size("inner")
    outer_count = lax.axis_size("outer")
    nhead = lax.axis_size("head")
    assert heads == n
    ib = n.bit_length() - 1
    ob = outer_count.bit_length() - 1
    lob = ob // 2
    hib = ob - lob
    nlo, nhi = 2**lob, 2**hib
    nb = ib + ob
    levels = level_weights.shape[0]
    assert levels == nb + 1
    gamma = DK ** (-0.5)
    scales = [rows ** (-0.5)] + [gamma * (rows * 2 ** (num - 1)) ** (-0.5) for num in range(1, levels)]
    dims = (n, nlo, nhi, nhead, ib, lob, hib, rows, tuple(scales), gamma)
    half = n // 2
    ibx = max(ib - 1, 1)
    any_spec = pl.BlockSpec(memory_space=pl.ANY)
    dma = pltpu.SemaphoreType.DMA

    def low(*shape):
        return pltpu.VMEM(shape, BF16)

    def wide(*shape):
        return pltpu.VMEM(shape, F32)

    sq = (DK, DK)
    scratch = [
        low(n, rows, DK), low(n, rows, DK), low(n, rows, DK), low(n, rows, DK), low(levels, rows),
        low(n, *sq), low(n, *sq), low(n, nb * DK, DK), low(ibx, max(n // 4, 1), *sq),
        low(*sq), low(nlo, *sq), low(*sq), low(nhi, *sq),
        wide(levels, rows, DK), low(n, rows, nb * DK), low(n, rows, rows), wide(n, rows, DK),
        low(n, rows, DK), low(n, nb, *sq),
        low(n, *sq), low(ibx, n, *sq), low(2, ob, half, *sq), low(hib, *sq), low(nhi, *sq),
        low(lob + 1, *sq), low(nlo, *sq), low(n, *sq), low(n, *sq), low(n, *sq),
        low(n, rows, DK), low(n, rows, DK), low(n, rows, DK),
        wide(levels, rows, DK), wide(levels, rows), wide(levels, rows),
        dma((4, n)), dma(()), dma((3, n)), dma(()), dma(()),
        dma((n,)), dma((n,)), dma((2,)), dma((ibx, n)), dma((ibx, n)),
        dma((nlo,)), dma((nlo,)), dma((nhi,)), dma((nhi,)), dma((2, ob, half)), dma((2, ob, half)),
        dma((2,)), dma((ibx, n)), dma((ibx, n)), dma((2, ob, half)), dma((2, ob, half)),
        dma((nhi,)), dma((nhi,)), dma((nlo,)), dma((nlo,)), dma((n,)), dma((n,)), dma((2,)),
    ]
    big = jax.ShapeDtypeStruct((rows, width), BF16)
    part_q, part_k, part_v, part_l, adjoints = pl.pallas_call(
        functools.partial(kernel, dims),
        out_shape=(
            big, big, big, jax.ShapeDtypeStruct((levels, rows), F32), jax.ShapeDtypeStruct((n, *sq), BF16)
        ),
        in_specs=[any_spec] * 5,
        out_specs=[any_spec] * 5,
        scratch_shapes=scratch,
        compiler_params=pltpu.CompilerParams(
            collective_id=0, has_side_effects=True, vmem_limit_bytes=60 * 2**20
        ),
        name="log_linear",
    )(queries, key_rows, value_rows, teacher_out, level_weights)
    return pl.pallas_call(
        functools.partial(finish_kernel, n),
        out_shape=(big, big, big, jax.ShapeDtypeStruct((levels, rows), F32)),
        in_specs=[any_spec] * 7,
        out_specs=[any_spec] * 4,
        scratch_shapes=[low(n, rows, DK) for _ in range(5)]
        + [wide(levels, rows), low(n, *sq), low(n, rows, DK), low(n, rows, DK)]
        + [dma((5, n)), dma((3, n)), dma(()), dma((2,))],
        compiler_params=pltpu.CompilerParams(vmem_limit_bytes=60 * 2**20),
        name="finish",
    )(part_q, part_k, part_v, key_rows, value_rows, part_l, adjoints)


def solution(mesh):
    tokens = P(("outer", "inner"), "head")
    per_token = P(None, ("outer", "inner"))
    return jax.shard_map(
        on_device,
        mesh=mesh,
        in_specs=(tokens, tokens, tokens, tokens, per_token),
        out_specs=(tokens, tokens, tokens, per_token),
        check_vma=False,
    )
```

```python
import functools

import jax
import jax.numpy as jnp
from jax import lax
from jax.experimental import pallas as pl
from jax.experimental.pallas import tpu as pltpu
from jax.sharding import PartitionSpec as P

DK = 128
MESH = pl.DeviceIdType.MESH
F32 = jnp.float32
BF16 = jnp.bfloat16


def nn(a, b):
    return lax.dot_general(a, b, (((1,), (0,)), ((), ())), preferred_element_type=F32)


def nt(a, b):
    return lax.dot_general(a, b, (((1,), (1,)), ((), ())), preferred_element_type=F32)


def tn(a, b):
    return lax.dot_general(a, b, (((0,), (0,)), ((), ())), preferred_element_type=F32)


def bit_of(number, position):
    return lax.rem(lax.div(number, 2**position), 2)


def kernel(
    dims,
    q_hbm, k_hbm, v_hbm, y_hbm, w_hbm,
    gq_hbm, gk_hbm, gv_hbm, gl_hbm, ba_hbm,
    Q, K, V, Y, W, BS, FR, LS, IS, TOT, YR, YT, XR, COEF, QC, SC, IN, ER, AD,
    AL1, AI, RP, BXS, BXR, BYS, BYR, DS, BA, DA, OQ, OK, OV, GACC, GLP, GLR,
    in_sem, w_sem, out_sem, gl_sem, ba_sem,
    f1s, f1r, fl1, f2s, f2r, fys, fyr, fxs, fxr, f3s, f3r,
    bl1, b2s, b2r, b3s, b3r, bxs, bxr, bys, byr, b4s, b4r, glx,
):
    n, nlo, nhi, nhead, ib, lob, hib, rows, scales, gamma = dims
    ob = lob + hib
    nb = ib + ob
    half = n // 2
    p = lax.axis_index("inner")
    g = lax.axis_index("outer")
    hd = lax.axis_index("head")
    x = lax.div(g, nlo)
    y = lax.rem(g, nlo)

    def zdev(r):
        return (hd, g, r)

    def odev(o):
        return (hd, o, p)

    def ydev(yy):
        return odev(x * nlo + yy)

    def xdev(xx):
        return odev(xx * nlo + y)

    def wrap(i):
        return lax.rem(i + 2 * n, n)

    def loop(count, body, unroll=1):
        def step(i, c):
            body(i)
            return c
        lax.fori_loop(0, count, step, 0, unroll=unroll)

    def rc(src, dst, ss, rs, dev):
        return pltpu.make_async_remote_copy(
            src_ref=src, dst_ref=dst, send_sem=ss, recv_sem=rs, device_id=dev, device_id_type=MESH
        )

    def cols(h):
        return pl.ds(pl.multiple_of(h * DK, DK), DK)

    def lev(b):
        return pl.ds(b * DK, DK)

    def in_copy(a, h):
        hbm, vm = ((k_hbm, K), (v_hbm, V), (q_hbm, Q), (y_hbm, Y))[a]
        return pltpu.make_async_copy(hbm.at[:, cols(h)], vm.at[h], in_sem.at[a, h])

    def out_copy(a, h):
        hbm, vm = ((gq_hbm, OQ), (gk_hbm, OK), (gv_hbm, OV))[a]
        return pltpu.make_async_copy(vm.at[h], hbm.at[:, cols(h)], out_sem.at[a, h])

    def start_kv(h):
        in_copy(0, h).start()
        in_copy(1, h).start()

    def start_qy(h):
        in_copy(2, h).start()
        in_copy(3, h).start()

    loop(n, start_kv)
    w_copy = pltpu.make_async_copy(w_hbm, W, w_sem)
    w_copy.start()
    loop(n, start_qy)

    barrier = pltpu.get_barrier_semaphore()

    def greet(dev):
        pl.semaphore_signal(barrier, inc=1, device_id=dev, device_id_type=MESH)

    loop(n - 1, lambda i: greet(zdev(wrap(p + 1 + i))))
    loop(nlo - 1, lambda i: greet(ydev(lax.rem(y + 1 + i, nlo))))
    loop(nhi - 1, lambda i: greet(xdev(lax.rem(x + 1 + i, nhi))))
    if nhead == 2:
        greet((1 - hd, g, p))

    def state(h):
        in_copy(0, h).wait()
        in_copy(1, h).wait()
        BS[h] = tn(K[h], V[h]).astype(BF16)


    def f1(h, src):
        return rc(BS.at[h], FR.at[src], f1s.at[h], f1r.at[src], zdev(h))

    def nth(i):
        near = half - lax.div(i + 1, 2)
        return wrap(p + near * (1 - 2 * lax.rem(i, 2)))

    state(nth(0))
    if n > 2:
        state(nth(1))
    pl.semaphore_wait(barrier, (n - 1) + (nlo - 1) + (nhi - 1) + (nhead - 1))

    def f1_start(i):
        f1(nth(i), p).start()

        @pl.when(i + 2 < n)
        def _():
            state(nth(i + 2))

    loop(n - 1, f1_start)
    if n == 2:
        state(p)
    fl1_copy = rc(BS, LS.at[:, lev(0), :], fl1.at[0], fl1.at[1], zdev(wrap(p + 1)))
    low0 = bit_of(p, 0) == 0

    @pl.when(low0)
    def _():
        fl1_copy.start()

    FR[p] = BS[p]

    w_copy.wait()
    for b in range(nb):
        bit = bit_of(p, b) if b < ib else bit_of(g, b - ib)

        @pl.when(bit == 0)
        def _():
            LS[:, lev(b), :] = jnp.zeros((n, DK, DK), BF16)

    weights = W[...]
    pick = lax.broadcasted_iota(jnp.int32, (nb + 1, DK), 0)
    for num in range(nb + 1):
        COEF[num] = tn(weights, jnp.where(pick == num, 1.0, 0.0).astype(BF16)) * scales[num]
    GACC[...] = jnp.zeros_like(GACC)

    def lower():
        return lax.broadcasted_iota(jnp.int32, (rows, rows), 0) >= lax.broadcasted_iota(
            jnp.int32, (rows, rows), 1
        )

    def ahead(h):
        in_copy(2, h).wait()
        in_copy(3, h).wait()
        query = Q[h]
        scores = nt(query, K[h]) * gamma
        kept = jnp.where(lower(), scores, 0.0).astype(BF16)
        SC[h] = kept
        IN[h] = nn(kept, V[h])
        query32 = query.astype(F32)
        for b in range(nb):
            QC[h, :, lev(b)] = (query32 * COEF[b + 1]).astype(BF16)

    loop(n, ahead)

    def f1_wait(i):
        src = wrap(p + 1 + i)
        f1(src, src).wait_recv()

    loop(n - 1, f1_wait)
    states = [FR[i].astype(F32) for i in range(n)]
    total = sum(states[1:], states[0])
    TOT[...] = total.astype(BF16)
    for b in range(1, ib):
        for node in range(n // 2 ** (b + 1)):
            first = node * 2 ** (b + 1)
            members = states[first : first + 2**b]
            IS[b - 1, node] = sum(members[1:], members[0]).astype(BF16)
    YR[y] = TOT[...]

    def fy(j, src):
        return rc(TOT, YR.at[src], fys.at[j], fyr.at[src], ydev(lax.rem(y + 1 + j, nlo)))

    loop(nlo - 1, lambda j: fy(j, y).start())

    def f2(b, dst, src):
        node = lax.div(dst, 2 ** (b + 1))
        return rc(
            IS.at[b - 1, node], LS.at[src, lev(b), :], f2s.at[b - 1, dst], f2r.at[b - 1, src], zdev(dst)
        )

    for b in range(1, ib):
        def f2_start(i):
            dst = wrap(p + 1 + i)

            @pl.when(bit_of(dst, b) == 1)
            def _():
                f2(b, dst, p).start()

        loop(n - 1, f2_start)

        @pl.when(bit_of(p, b) == 1)
        def _():
            LS[p, lev(b), :] = IS[b - 1, lax.div(p, 2 ** (b + 1))]

    def masked_sum(ref, count, me, m):
        out = jnp.zeros((DK, DK), F32)
        for i in range(count):
            cond = (
                (bit_of(me, m) == 1)
                & (lax.div(me, 2 ** (m + 1)) == i >> (m + 1))
                & ((i >> m) % 2 == 0)
            )
            out = out + jnp.where(cond, ref[i].astype(F32), 0.0)
        return out

    def f3(way, m, s, head):
        dst = wrap(p + 1) if way == 0 else wrap(p - 1)
        rows_here = part(way) if s == half - 1 else (0, DK)
        slot = LS.at[head, pl.ds((ib + m) * DK + rows_here[0], rows_here[1]), :]
        return rc(slot, slot, f3s.at[way, m, s], f3r.at[way, m, s], zdev(dst))

    hops = half

    def part(way):
        return (way * (DK // 2), DK // 2)

    def on_bit(m, body):
        @pl.when(bit_of(g, m) == 1)
        def _():
            body()

    def f3_step(m, s):
        for way in range(2):
            if s > 0:
                head = wrap(p - s) if way == 0 else wrap(p + s)
                f3(way, m, s - 1, head).wait_recv()
            if s < hops:
                head = wrap(p - s) if way == 0 else wrap(p + s)
                f3(way, m, s, head).start()

    def fy_wait(j):
        src = lax.rem(y + 1 + j, nlo)
        fy(j, src).wait_recv()

    loop(nlo - 1, fy_wait)
    for m in range(lob):
        on_bit(m, lambda: LS.__setitem__((p, lev(ib + m)), masked_sum(YR, nlo, y, m).astype(BF16)))
    parts = [YR[i].astype(F32) for i in range(nlo)]
    YT[...] = sum(parts[1:], parts[0]).astype(BF16)
    for m in range(lob):
        on_bit(m, lambda: f3_step(m, 0))

    def fx(dst, src):
        return rc(YT, XR.at[src], fxs.at[dst], fxr.at[src], xdev(dst))

    def fx_start(j):
        @pl.when(x + 1 + j < nhi)
        def _():
            fx(x + 1 + j, x).start()

    def fx_wait(j):
        @pl.when(j < x)
        def _():
            fx(j, j).wait_recv()

    loop(nhi - 1, fx_start)
    for m in range(lob):
        on_bit(m, lambda: f3_step(m, 1))
    loop(nhi - 1, fx_wait)
    for m in range(hib):
        on_bit(lob + m, lambda: LS.__setitem__((p, lev(ib + lob + m)), masked_sum(XR, nhi, x, m).astype(BF16)))
    for m in range(hib):
        on_bit(lob + m, lambda: f3_step(lob + m, 0))

    @pl.when(bit_of(p, 0) == 1)
    def _():
        fl1_copy.wait_recv()

    def b2(b, dst, src):
        return rc(AD.at[dst, b], AI.at[b - 1, src], b2s.at[b - 1, dst], b2r.at[b - 1, src], zdev(dst))

    def finish(h):
        inter = nn(QC[h], LS[h])
        error = (COEF[0] * IN[h] + inter - Y[h].astype(F32)).astype(BF16)
        ER[h] = error
        adjoint = tn(error, QC[h]).astype(BF16)
        for b in range(nb):
            AD[h, b] = adjoint[:, b * DK : (b + 1) * DK]

    def far(h):
        for b in range(1, ib):
            @pl.when(bit_of(p, b) == 1)
            def _():
                f2(b, p, h).wait_recv()
        finish(h)

    finish(p)
    for b in range(1, ib):
        @pl.when(bit_of(p, b) == 1)
        def _():
            AI[b - 1, p] = AD[p, b]

    for s in range(1, half + 1):
        if s < half:
            for m in range(lob):
                on_bit(m, lambda: f3_step(m, s + 1))
        for m in range(lob, ob):
            on_bit(m, lambda: f3_step(m, s))
        heads = [wrap(p - s)] + ([wrap(p + s)] if s < half else [])
        def both(i):
            h = wrap(p - s + 2 * s * i)
            far(h)
        loop(len(heads), both)

    def b3(way, m, s):
        dst = wrap(p + 1) if way == 0 else wrap(p - 1)
        some_rows = pl.ds(*(part(way) if s == 0 else (0, DK)))
        return rc(
            AD.at[chained(way, s), ib + m, some_rows], RP.at[way, m, s, some_rows],
            b3s.at[way, m, s], b3r.at[way, m, s], zdev(dst),
        )

    def chained(way, s):
        return wrap(p + half - s) if way == 0 else wrap(p - half + s)

    def b3_step(m, s):
        for way in range(2):
            if s > 0:
                b3(way, m, s - 1).wait_recv()
                some_rows = pl.ds(*(part(way) if s == 1 else (0, DK)))
                head = chained(way, s)
                AD[head, ib + m, some_rows] = (
                    AD[head, ib + m, some_rows].astype(F32) + RP[way, m, s - 1, some_rows].astype(F32)
                ).astype(BF16)
            b3(way, m, s).start()

    for m in reversed(range(ob)):
        on_bit(m, lambda: b3_step(m, 0))

    bl1_copy = rc(AD.at[:, 0], AL1, bl1.at[0], bl1.at[1], zdev(wrap(p - 1)))

    def heavy(h):
        error = ER[h]
        error32 = error.astype(F32)
        query = Q[h]
        query32 = query.astype(F32)
        key = K[h]
        intra_error = (COEF[0] * error32).astype(BF16)
        raw = nt(intra_error, V[h]) * gamma
        score_grad = jnp.where(lower(), raw, 0.0).astype(BF16)
        back = nt(error, LS[h])
        grad = nn(score_grad, key)
        GACC[0] += error32 * IN[h]
        for b in range(nb):
            piece = back[:, b * DK : (b + 1) * DK]
            grad = grad + COEF[b + 1] * piece
            GACC[b + 1] += query32 * piece
        OQ[h] = grad.astype(BF16)
        OK[h] = tn(score_grad, query).astype(BF16)
        OV[h] = tn(SC[h], intra_error).astype(BF16)

    per_step = n // (half + 1) if half > 1 else 1
    done = 0

    def some(count):
        nonlocal done
        count = min(count, n - done)
        first = done
        if count > 0:
            loop(count, lambda i: heavy(first + i))
        done = first + count

    for s in range(1, half):
        some(per_step)
        for m in reversed(range(ob)):
            on_bit(m, lambda: b3_step(m, s))

    @pl.when(bit_of(p, 0) == 1)
    def _():
        bl1_copy.start()

    for b in reversed(range(1, ib)):
        @pl.when(bit_of(p, b) == 1)
        def _():
            loop(n - 1, lambda i: b2(b, wrap(p + 1 + i), p).start())

    some(per_step)

    def own(m):
        first, second = RP[0, m, half - 1].astype(F32), RP[1, m, half - 1].astype(F32)
        if half == 1:
            top = lax.broadcasted_iota(jnp.int32, (DK, DK), 0) < DK // 2
            return AD[p, ib + m].astype(F32) + jnp.where(top, first, second)
        return AD[p, ib + m].astype(F32) + first + second

    def own_wait(m):
        for way in range(2):
            b3(way, m, half - 1).wait_recv()
        if m >= lob:
            BXS[m - lob] = own(m).astype(BF16)

    for m in reversed(range(lob, ob)):
        on_bit(m, lambda: own_wait(m))

    def bx(m, dst, src):
        return rc(BXS.at[m], BXR.at[src], bxs.at[dst], bxr.at[src], xdev(dst))

    def top_bit(a, b, m):
        return (lax.div(a, 2 ** (m + 1)) == lax.div(b, 2 ** (m + 1))) & (
            lax.div(a, 2**m) != lax.div(b, 2**m)
        )

    for j in range(nhi - 1):
        for m in range(hib):
            @pl.when((j < x) & top_bit(x, jnp.int32(j), m))
            def _():
                bx(m, j, x).start()

    for m in range(lob):
        on_bit(m, lambda: own_wait(m))
    some(1)

    for j in range(1, nhi):
        @pl.when(j > x)
        def _():
            bx(0, 0, j).wait_recv()

    outer = jnp.zeros((DK, DK), F32)
    for j in range(1, nhi):
        outer = outer + jnp.where(j > x, BXR[j].astype(F32), 0.0)
    BYS[0] = outer.astype(BF16)
    for m in range(lob):
        @pl.when(bit_of(y, m) == 1)
        def _():
            BYS[m + 1] = (outer + own(m)).astype(BF16)

    def by(kind, dst, src):
        return rc(BYS.at[kind], BYR.at[src], bys.at[dst], byr.at[src], ydev(dst))

    for j in range(nlo):
        @pl.when(j > y)
        def _():
            by(0, j, y).start()
        for m in range(lob):
            @pl.when((j < y) & top_bit(y, jnp.int32(j), m))
            def _():
                by(m + 1, j, y).start()

    some(1)

    for b in range(1, ib):
        def b2_wait(i):
            src = wrap(p + 1 + i)

            @pl.when(bit_of(src, b) == 1)
            def _():
                b2(b, src, src).wait_recv()

        loop(n - 1, b2_wait)

    for j in range(nlo):
        @pl.when(j != y)
        def _():
            by(0, j, j).wait_recv()
    for j in range(nlo):
        outer = outer + jnp.where(j != y, BYR[j].astype(F32), 0.0)
    nodes = {}
    for b in range(1, ib):
        for node in range(n // 2 ** (b + 1)):
            first = node * 2 ** (b + 1) + 2**b
            members = [AI[b - 1, c].astype(F32) for c in range(first, first + 2**b)]
            nodes[b, node] = sum(members[1:], members[0])
    for dst in range(n):
        value = outer
        for b in range(1, ib):
            if (dst >> b) % 2 == 0:
                value = value + nodes[b, dst >> (b + 1)]
        DS[dst] = value.astype(BF16)
    BA[p] = DS[p]

    def b4(dst, src):
        return rc(DS.at[dst], BA.at[src], b4s.at[dst], b4r.at[src], zdev(dst))

    loop(half, lambda i: b4(wrap(p + half + i), p).start())
    loop(half - 1, lambda i: b4(wrap(p + 1 + i), p).start())
    some(n)

    row = lax.broadcasted_iota(jnp.int32, (nb + 1, rows), 0)
    ones = jnp.ones((nb + 1, DK), F32)
    mine = jnp.zeros((nb + 1, rows), F32)
    for num in range(nb + 1):
        sums = lax.dot_general(
            ones, GACC[num], (((1,), (1,)), ((), ())),
            precision=lax.Precision.HIGHEST, preferred_element_type=F32,
        )
        mine = jnp.where(row == num, sums * scales[num], mine)
    GLP[...] = mine

    def write(h):
        for a in range(3):
            out_copy(a, h).start()

    loop(n, write)
    if nhead == 2:
        glx_copy = rc(GLP, GLR, glx.at[0], glx.at[1], (1 - hd, g, p))
        glx_copy.start()

    @pl.when(low0)
    def _():
        bl1_copy.wait_recv()

    def last(i):
        h = wrap(p + i)

        @pl.when(i > 0)
        def _():
            b4(h, h).wait_recv()
        adjoint = BA[h].astype(F32) + jnp.where(low0, AL1[h].astype(F32), 0.0)
        DA[h] = adjoint.astype(BF16)

    loop(n, last)
    ba_copy = pltpu.make_async_copy(DA, ba_hbm, ba_sem)
    ba_copy.start()

    if nhead == 2:
        glx_copy.wait_recv()
        glx_copy.wait_send()
        GLP[...] = GLP[...] + GLR[...]
    gl_copy = pltpu.make_async_copy(GLP, gl_hbm, gl_sem)
    gl_copy.start()

    loop(n - 1, lambda i: f1(wrap(p + 1 + i), p).wait_send())

    @pl.when(low0)
    def _():
        fl1_copy.wait_send()

    @pl.when(bit_of(p, 0) == 1)
    def _():
        bl1_copy.wait_send()

    loop(nlo - 1, lambda j: fy(j, y).wait_send())

    def fx_sent(j):
        @pl.when(x + 1 + j < nhi)
        def _():
            fx(x + 1 + j, x).wait_send()

    loop(nhi - 1, fx_sent)
    for b in range(1, ib):
        def sent(i):
            dst = wrap(p + 1 + i)

            @pl.when(bit_of(dst, b) == 1)
            def _():
                f2(b, dst, p).wait_send()

            @pl.when(bit_of(p, b) == 1)
            def _():
                b2(b, dst, p).wait_send()

        loop(n - 1, sent)
    for m in range(ob):
        def chain_sent():
            for way in range(2):
                for s in range(hops):
                    f3(way, m, s, wrap(p - s) if way == 0 else wrap(p + s)).wait_send()
                    b3(way, m, s).wait_send()
        on_bit(m, chain_sent)
    for j in range(nhi - 1):
        @pl.when(j < x)
        def _():
            bx(0, j, x).wait_send()
    for j in range(nlo):
        @pl.when(j != y)
        def _():
            by(0, j, y).wait_send()
    loop(n - 1, lambda i: b4(wrap(p + 1 + i), p).wait_send())

    def written(h):
        for a in range(3):
            out_copy(a, h).wait()

    loop(n, written)
    gl_copy.wait()
    ba_copy.wait()


def finish_kernel(
    n, pq_hbm, pk_hbm, pv_hbm, k_hbm, v_hbm, pl_hbm, a_hbm, gq_hbm, gk_hbm, gv_hbm, gl_hbm,
    GQ, PK, PV, K, V, GL, A, GK, GV, in_sem, out_sem, a_sem, l_sem,
):
    def loop(body):
        def step(i, c):
            body(i)
            return c
        lax.fori_loop(0, n, step, 0)

    def cols(h):
        return pl.ds(pl.multiple_of(h * DK, DK), DK)

    ins = ((pq_hbm, GQ), (pk_hbm, PK), (pv_hbm, PV), (k_hbm, K), (v_hbm, V))
    outs = ((gq_hbm, GQ), (gk_hbm, GK), (gv_hbm, GV))

    def in_copy(a, h):
        return pltpu.make_async_copy(ins[a][0].at[:, cols(h)], ins[a][1].at[h], in_sem.at[a, h])

    def out_copy(a, h):
        return pltpu.make_async_copy(outs[a][1].at[h], outs[a][0].at[:, cols(h)], out_sem.at[a, h])

    a_copy = pltpu.make_async_copy(a_hbm, A, a_sem)
    a_copy.start()
    l_copy = pltpu.make_async_copy(pl_hbm, GL, l_sem.at[0])
    l_copy.start()

    def start(h):
        for a in (4, 1, 3, 2, 0):
            in_copy(a, h).start()

    loop(start)
    l_copy.wait()
    l_out = pltpu.make_async_copy(GL, gl_hbm, l_sem.at[1])
    l_out.start()
    a_copy.wait()

    def one(h):
        for a in (4, 1, 3, 2, 0):
            in_copy(a, h).wait()
        out_copy(0, h).start()
        adjoint = A[h]
        GK[h] = (PK[h].astype(F32) + nn(V[h], adjoint)).astype(BF16)
        GV[h] = (PV[h].astype(F32) + nt(K[h], adjoint)).astype(BF16)
        out_copy(1, h).start()
        out_copy(2, h).start()

    loop(one)

    def done(h):
        for a in range(3):
            out_copy(a, h).wait()

    loop(done)
    l_out.wait()


def on_device(queries, key_rows, value_rows, teacher_out, level_weights):
    rows, width = queries.shape
    heads = width // DK
    n = lax.axis_size("inner")
    outer_count = lax.axis_size("outer")
    nhead = lax.axis_size("head")
    assert heads == n
    ib = n.bit_length() - 1
    ob = outer_count.bit_length() - 1
    lob = ob // 2
    hib = ob - lob
    nlo, nhi = 2**lob, 2**hib
    nb = ib + ob
    levels = level_weights.shape[0]
    assert levels == nb + 1
    gamma = DK ** (-0.5)
    scales = [rows ** (-0.5)] + [gamma * (rows * 2 ** (num - 1)) ** (-0.5) for num in range(1, levels)]
    dims = (n, nlo, nhi, nhead, ib, lob, hib, rows, tuple(scales), gamma)
    half = n // 2
    ibx = max(ib - 1, 1)
    any_spec = pl.BlockSpec(memory_space=pl.ANY)
    dma = pltpu.SemaphoreType.DMA

    def low(*shape):
        return pltpu.VMEM(shape, BF16)

    def wide(*shape):
        return pltpu.VMEM(shape, F32)

    sq = (DK, DK)
    scratch = [
        low(n, rows, DK), low(n, rows, DK), low(n, rows, DK), low(n, rows, DK), low(levels, rows),
        low(n, *sq), low(n, *sq), low(n, nb * DK, DK), low(ibx, max(n // 4, 1), *sq),
        low(*sq), low(nlo, *sq), low(*sq), low(nhi, *sq),
        wide(levels, rows, DK), low(n, rows, nb * DK), low(n, rows, rows), wide(n, rows, DK),
        low(n, rows, DK), low(n, nb, *sq),
        low(n, *sq), low(ibx, n, *sq), low(2, ob, half, *sq), low(hib, *sq), low(nhi, *sq),
        low(lob + 1, *sq), low(nlo, *sq), low(n, *sq), low(n, *sq), low(n, *sq),
        low(n, rows, DK), low(n, rows, DK), low(n, rows, DK),
        wide(levels, rows, DK), wide(levels, rows), wide(levels, rows),
        dma((4, n)), dma(()), dma((3, n)), dma(()), dma(()),
        dma((n,)), dma((n,)), dma((2,)), dma((ibx, n)), dma((ibx, n)),
        dma((nlo,)), dma((nlo,)), dma((nhi,)), dma((nhi,)), dma((2, ob, half)), dma((2, ob, half)),
        dma((2,)), dma((ibx, n)), dma((ibx, n)), dma((2, ob, half)), dma((2, ob, half)),
        dma((nhi,)), dma((nhi,)), dma((nlo,)), dma((nlo,)), dma((n,)), dma((n,)), dma((2,)),
    ]
    big = jax.ShapeDtypeStruct((rows, width), BF16)
    part_q, part_k, part_v, part_l, adjoints = pl.pallas_call(
        functools.partial(kernel, dims),
        out_shape=(
            big, big, big, jax.ShapeDtypeStruct((levels, rows), F32), jax.ShapeDtypeStruct((n, *sq), BF16)
        ),
        in_specs=[any_spec] * 5,
        out_specs=[any_spec] * 5,
        scratch_shapes=scratch,
        compiler_params=pltpu.CompilerParams(
            collective_id=0, has_side_effects=True, vmem_limit_bytes=60 * 2**20
        ),
        name="log_linear",
    )(queries, key_rows, value_rows, teacher_out, level_weights)
    return pl.pallas_call(
        functools.partial(finish_kernel, n),
        out_shape=(big, big, big, jax.ShapeDtypeStruct((levels, rows), F32)),
        in_specs=[any_spec] * 7,
        out_specs=[any_spec] * 4,
        scratch_shapes=[low(n, rows, DK) for _ in range(5)]
        + [wide(levels, rows), low(n, *sq), low(n, rows, DK), low(n, rows, DK)]
        + [dma((5, n)), dma((3, n)), dma(()), dma((2,))],
        compiler_params=pltpu.CompilerParams(vmem_limit_bytes=60 * 2**20),
        name="finish",
    )(part_q, part_k, part_v, key_rows, value_rows, part_l, adjoints)


def solution(mesh):
    tokens = P(("outer", "inner"), "head")
    per_token = P(None, ("outer", "inner"))
    return jax.shard_map(
        on_device,
        mesh=mesh,
        in_specs=(tokens, tokens, tokens, tokens, per_token),
        out_specs=(tokens, tokens, tokens, per_token),
        check_vma=False,
    )
```
